32 devices in a mesh: gx: 4 (over z), gy: 2 (over core), gz: 4 (over y, x).
Axes of the slice: x: 2, y: 2, z: 4, core: 2. Of those that a mesh axis runs over, the one named last changes fastest.
Arguments:
- pair: bfloat16 [128, 512, 512], P('gz', 'gx', 'gy'), may hold values from -6 to 6
- pair_mask: int32 [512, 512], P('gx', 'gy'), may hold values from 0 to 1, as said below
- input_gain: float32 [128], replicated, may hold values from 0.1 to 1.9
- input_weights: bfloat16 [4, 128, 128], replicated, may hold values from -0.5 to 0.5
- out_gate_weight: bfloat16 [128, 128], replicated, may hold values from -0.5 to 0.5
- hidden_gain: float32 [128], replicated, may hold values from 0.1 to 1.9
- out_weight: bfloat16 [128, 128], replicated, may hold values from -0.5 to 0.5
Outputs:
- update: bfloat16 [128, 512, 512], P('gz', 'gx', 'gy')
The draws below stay inside these ranges and needn't reach their ends.
Inputs may be any that keep to these rules, and one draw needn't show every extreme that they name: pair_mask[r, s] = m[r] * m[s] for a 0/1 residue mask m of the draw that is 0 for all r >= L, for one crop length L with 256 < L <= 512; residues below L may also be 0.
All inputs are finite; a program needn't handle non-finite values.
Results may differ from the reference program's by a relative error of at most 0.011.
Values may be sent and summed in bfloat16 or wider, within the bound.
A program may use at most 64 MiB of HBM per device.

```python
import jax
import jax.numpy as jnp
from jax import lax

C = 128
CH = 128
N = 512


def draw_pair_mask(key, part):
    crop_length = jax.random.randint(jax.random.fold_in(key, 7), (), N // 2 + 1, N + 1)
    dropped = jax.random.randint(jax.random.fold_in(key, 11), (N,), 0, 16)
    inside = ((jnp.arange(N) < crop_length) & (dropped != 0)).astype(jnp.int32)
    return inside[:, None] * inside[None, :]


def levels(own_key, extent, split, least, largest):
    loudness, own = 1.0, jax.random.fold_in(own_key, 6)
    for axis_at, shards_of in split:
        steps = jnp.exp(jax.random.uniform(jax.random.fold_in(own, axis_at), (shards_of,), jnp.float32, least / len(split), largest / len(split)))
        loudness = loudness * jnp.repeat(steps, extent[axis_at] // shards_of).reshape([-1 if axis == axis_at else 1 for axis in range(len(extent))])
    return loudness


def bell_draw(stream_key, shape, width, most, cuts=(), kind=jnp.bfloat16):
    factor_of = levels(stream_key, shape, cuts, -0.22, 0.18) if cuts else 1.0
    result = jax.random.normal(stream_key, shape, jnp.float32) * width * factor_of
    return jnp.minimum(jnp.maximum(result, -most), most).astype(kind)


def setup_inputs(seed: int = 0) -> dict:
    seeds = jax.random.split(jax.random.key(seed), 8)
    pair = bell_draw(seeds[0], (C, N, N), 1.0, 6.0, ((0, 4), (1, 4), (2, 2)))
    pair_mask = draw_pair_mask(jax.random.fold_in(seeds[7], 71), 0)
    input_gain = jnp.clip(1.0 + 0.18 * jax.random.normal(seeds[2], (C,), jnp.float32), 0.1, 1.9)
    input_weights = bell_draw(seeds[3], (4, C, CH), C ** -0.5, 0.5)
    out_gate_weight = bell_draw(seeds[4], (C, C), C ** -0.5, 0.5)
    hidden_gain = jnp.clip(1.0 + 0.18 * jax.random.normal(seeds[5], (CH,), jnp.float32), 0.1, 1.9)
    out_weight = bell_draw(seeds[6], (CH, C), CH ** -0.5, 0.5)
    return dict(pair=pair, pair_mask=pair_mask, input_gain=input_gain, input_weights=input_weights, out_gate_weight=out_gate_weight, hidden_gain=hidden_gain, out_weight=out_weight)


EPSILON = 1e-05

def layer_norm(values, gains):
    average = lax.optimization_barrier(jnp.mean(values, axis=0))
    spread = lax.optimization_barrier(jnp.mean(jnp.square(values - average), axis=0))
    return (values - average) * lax.rsqrt(spread + EPSILON) * gains[:, None, None]

def project(weights, normed):
    return jnp.einsum('dk,drs->krs', weights.astype(jnp.float32), normed.astype(jnp.float32))

def reference(pair, pair_mask, input_gain, input_weights, out_gate_weight, hidden_gain, out_weight):
    normed = layer_norm(pair.astype(jnp.float32), input_gain).astype(jnp.bfloat16)
    mask_values = pair_mask.astype(jnp.float32)
    left_side = (mask_values * jax.nn.sigmoid(project(input_weights[0], normed)) * project(input_weights[1], normed)).astype(jnp.bfloat16)
    right_side = (mask_values * jax.nn.sigmoid(project(input_weights[2], normed)) * project(input_weights[3], normed)).astype(jnp.bfloat16)
    gate = jax.nn.sigmoid(project(out_gate_weight, normed))
    triangle = jnp.einsum('hki,hkj->hij', left_side.astype(jnp.float32), right_side.astype(jnp.float32))
    hidden_normed = layer_norm(triangle, hidden_gain).astype(jnp.bfloat16)
    projected = project(out_weight, hidden_normed)
    return (mask_values * gate * projected).astype(jnp.bfloat16)
```

```python
import functools

import jax
import jax.numpy as jnp
from jax import lax
from jax.experimental import pallas as pl
from jax.experimental.pallas import tpu as pltpu
from jax.sharding import PartitionSpec as P

EPSILON = 1e-05
MESH = pl.DeviceIdType.MESH


def position(axes):
    at = 0
    for name in axes:
        at = at * lax.axis_size(name) + lax.axis_index(name)
    return at


def coordinates(axes, at):
    where = {}
    for name in reversed(axes):
        where[name] = lax.rem(at, lax.axis_size(name))
        at = at // lax.axis_size(name)
    return where


ROWS = 8
LANES = 128


def panels(span):
    return [(at, slice(at * LANES, (at + 1) * LANES)) for at in range(span // LANES)]


def row_of(store, row, height, span):
    parts = [store[at, pl.ds(row, height, stride=ROWS), :] for at, _ in panels(span)]
    return jnp.concatenate(parts, axis=1)


def put_row(store, row, height, span, value):
    for at, lanes in panels(span):
        store[at, pl.ds(row, height, stride=ROWS), :] = value[:, lanes]


def pack(store, target, span):
    for at, lanes in panels(span):
        height = store.shape[1] // ROWS
        target[:, :, lanes] = store[at].reshape(height, ROWS, LANES).astype(jnp.bfloat16)


def greet(groups):
    barrier = pltpu.get_barrier_semaphore()
    total = 0
    for axes, count in groups:
        me = position(axes)

        @pl.loop(1, count)
        def _(step):
            there = coordinates(axes, lax.rem(me + step, count))
            pl.semaphore_signal(barrier, inc=1, device_id=there, device_id_type=MESH)

        total += count - 1
    pl.semaphore_wait(barrier, total)


def standardize(values, plain):
    average = jnp.sum(values, axis=0) / values.shape[0]
    centred = values - average
    spread = jnp.sum(centred * centred, axis=0) / values.shape[0]
    result = centred * lax.rsqrt(spread + EPSILON)
    for at, lanes in panels(values.shape[2]):
        plain[at] = result[:, :, lanes].reshape(plain.shape[1:])


def wrapped(at, step, count):
    moved = at + step
    return jnp.where(moved >= count, moved - count, moved)


def whole_kernel(
    flat, count, quads, split, pair, far_mask, far_input_gain, far_input_weights, far_gate_weight, far_hidden_gain,
    far_out_weight,
    update,
    mask, input_gain, input_weights, out_gate_weight, hidden_gain, out_weight, fetched,
    turned, spread_gain, wide_left, far_right, half_left, half_right, gate, triangle,
    landed, plain, sided, outgoing, returned, finished,
    pair_send, pair_recv, pair_own, sends, receives, half_sends, half_receives, gsend, greceive, own,
    back_send, back_recv, out_send, out_recv, out_own,
):
    whole_depth, half_depth = split
    depth = whole_depth + half_depth
    me = position(flat)
    quad = lax.axis_index("gz")
    core = lax.axis_index("gy")
    cores = lax.axis_size("gy")
    chunks, channels, _, span = landed.shape
    local = pair.shape[0]
    rows = chunks * ROWS
    hidden = outgoing.shape[2]
    members = count // 2
    half = lax.div(me, members)
    member = me - half * members
    base = half * members

    fetches = [
        pltpu.make_async_copy(source, target, fetched.at[at])
        for at, (source, target) in enumerate((
            (far_input_weights, input_weights), (far_input_gain, input_gain), (far_mask, mask),
            (far_gate_weight, out_gate_weight), (far_hidden_gain, hidden_gain), (far_out_weight, out_weight),
        ))
    ]
    for fetch in fetches:
        fetch.start()

    greet(((flat, count), (("gy",), cores)))

    def chip(at):
        across = lax.div(at, quads)
        return {"gx": across, "gz": at - across * quads}

    def wide_gain(at):
        return jnp.concatenate([spread_gain[at]] * (span // LANES), axis=1)

    def inside_of(chunk, row):
        first = quad * rows + chunk * ROWS + row
        return mask[pl.ds(first, 1), :].astype(jnp.float32)

    columns = pl.ds(pl.multiple_of(core * span, span), span)

    def pair_copy(chunk, step, sender, target):
        first = pl.multiple_of(target * rows + chunk * ROWS, ROWS)
        return pltpu.make_async_remote_copy(
            src_ref=pair.at[:, pl.ds(first, ROWS), :],
            dst_ref=landed.at[chunk, pl.ds(sender * local, local)],
            send_sem=pair_send.at[chunk, step],
            recv_sem=pair_recv.at[chunk, step],
            device_id={"gz": target},
            device_id_type=MESH,
        )

    def pair_keep(chunk):
        first = pl.multiple_of(quad * rows + chunk * ROWS, ROWS)
        return pltpu.make_async_copy(
            pair.at[:, pl.ds(first, ROWS), :],
            landed.at[chunk, pl.ds(quad * local, local)],
            pair_own.at[chunk],
        )

    def cut_of(chunk):
        return pl.ds(pl.multiple_of(chunk * ROWS, ROWS), ROWS)

    def landing(side, chunk, sender):
        if side == 0:
            return wide_left.at[:, sender, cut_of(chunk), columns]
        return far_right.at[:, sender, cut_of(chunk), :]

    def half_landing(side, chunk, sender):
        if side == 0:
            return half_left.at[:, sender, cut_of(chunk), columns]
        return half_right.at[:, sender, cut_of(chunk), :]

    def copy(side, chunk, step, sender, target):
        return pltpu.make_async_remote_copy(
            src_ref=outgoing.at[side, chunk, pl.ds(target * whole_depth, whole_depth)],
            dst_ref=landing(side, chunk, sender),
            send_sem=sends.at[side, chunk, step],
            recv_sem=receives.at[side, chunk, step],
            device_id=chip(target),
            device_id_type=MESH,
        )

    def half_part(target):
        return pl.ds(count * whole_depth + target * half_depth, half_depth)

    def half_copy(side, chunk, step, sender, target):
        return pltpu.make_async_remote_copy(
            src_ref=outgoing.at[side, chunk, half_part(target)],
            dst_ref=half_landing(side, chunk, sender),
            send_sem=half_sends.at[side, chunk, step],
            recv_sem=half_receives.at[side, chunk, step],
            device_id=chip(base + target),
            device_id_type=MESH,
        )

    def keep(side, chunk):
        return pltpu.make_async_copy(
            outgoing.at[side, chunk, pl.ds(me * whole_depth, whole_depth)],
            landing(side, chunk, me),
            own.at[0, side, chunk],
        )

    def half_keep(side, chunk):
        return pltpu.make_async_copy(
            outgoing.at[side, chunk, half_part(member)],
            half_landing(side, chunk, member),
            own.at[1, side, chunk],
        )

    def passed(chunk, ahead):
        where = {"gy": lax.rem(core + ahead, cores)}
        made = []
        for at, (store, used) in enumerate(((wide_left, whole_depth), (half_left, half_depth))):
            if used:
                made.append(pltpu.make_async_remote_copy(
                    src_ref=store.at[:, :, cut_of(chunk), columns],
                    dst_ref=store.at[:, :, cut_of(chunk), columns],
                    send_sem=gsend.at[at, chunk, ahead],
                    recv_sem=greceive.at[at, chunk, ahead],
                    device_id=where,
                    device_id_type=MESH,
                ))
        return made

    def send(side, chunk):
        if whole_depth:
            @pl.loop(1, count)
            def _(step):
                copy(side, chunk, step, me, wrapped(me, step, count)).start()

            keep(side, chunk).start()
        if half_depth:
            @pl.loop(1, members)
            def _(step):
                half_copy(side, chunk, step, member, wrapped(member, step, members)).start()

            half_keep(side, chunk).start()

    def receive(side, chunk):
        if whole_depth:
            @pl.loop(1, count)
            def _(step):
                copy(side, chunk, step, wrapped(me, count - step, count), wrapped(me, step, count)).wait()

            keep(side, chunk).wait()
        if half_depth:
            @pl.loop(1, members)
            def _(step):
                half_copy(
                    side, chunk, step, wrapped(member, members - step, members), wrapped(member, step, members)
                ).wait()

            half_keep(side, chunk).wait()

    @pl.loop(0, chunks)
    def _(chunk):
        pair_keep(chunk).start()

        @pl.loop(1, quads)
        def _(step):
            pair_copy(chunk, step, quad, wrapped(quad, step, quads)).start()

    for fetch in fetches:
        fetch.wait()
    for at in range(4):
        turned[at] = input_weights[at].astype(jnp.float32).T.astype(jnp.bfloat16)
    turned[4] = out_gate_weight[...].astype(jnp.float32).T.astype(jnp.bfloat16)
    turned[5] = out_weight[...].astype(jnp.float32).T.astype(jnp.bfloat16)
    spread_gain[0] = jnp.broadcast_to(input_gain[...], (LANES, channels)).T
    spread_gain[1] = jnp.broadcast_to(hidden_gain[...], (LANES, hidden)).T

    @pl.loop(0, chunks)
    def _(chunk):
        @pl.loop(1, quads)
        def _(step):
            pair_copy(chunk, step, wrapped(quad, quads - step, quads), wrapped(quad, step, quads)).wait()

        pair_keep(chunk).wait()
        standardize(landed[chunk].astype(jnp.float32), plain)

        def normed_row(row):
            return (row_of(plain, row, channels, span) * wide_gain(0)).astype(jnp.bfloat16)

        def product(at, normed):
            return jnp.dot(turned[at], normed, preferred_element_type=jnp.float32)

        for side in range(2):
            @pl.loop(0, ROWS)
            def _(row):
                normed = normed_row(row)
                gating = inside_of(chunk, row) * jax.nn.sigmoid(product(2 * side, normed))
                put_row(sided.at[side], row, hidden, span, gating * product(2 * side + 1, normed))

            pack(sided.at[side], outgoing.at[side, chunk], span)
            send(side, chunk)

        @pl.loop(0, ROWS)
        def _(row):
            gate[chunk * ROWS + row] = jax.nn.sigmoid(product(4, normed_row(row)))

    @pl.loop(0, chunks)
    def _(chunk):
        for side in range(2):
            receive(side, chunk)
            if side == 0:
                for ahead in range(1, cores):
                    for made in passed(chunk, ahead):
                        made.start()

    @pl.loop(0, chunks)
    def _(chunk):
        for ahead in range(1, cores):
            for made in passed(chunk, ahead):
                made.wait()

    def back_copy(chunk, step, sender, target):
        return pltpu.make_async_remote_copy(
            src_ref=triangle.at[:, target, chunk],
            dst_ref=returned.at[chunk, sender],
            send_sem=back_send.at[chunk, step],
            recv_sem=back_recv.at[chunk, step],
            device_id=chip(target),
            device_id_type=MESH,
        )

    def out_copy(chunk, step, sender, target):
        first = pl.multiple_of(sender * rows + chunk * ROWS, ROWS)
        return pltpu.make_async_remote_copy(
            src_ref=finished.at[chunk, pl.ds(target * local, local)],
            dst_ref=update.at[:, pl.ds(first, ROWS), :],
            send_sem=out_send.at[chunk, step],
            recv_sem=out_recv.at[chunk, step],
            device_id={"gz": target},
            device_id_type=MESH,
        )

    def out_keep(chunk):
        first = pl.multiple_of(quad * rows + chunk * ROWS, ROWS)
        return pltpu.make_async_copy(
            finished.at[chunk, pl.ds(quad * local, local)],
            update.at[:, pl.ds(first, ROWS), :],
            out_own.at[chunk],
        )

    def multiply(left, right):
        product = lax.dot_general(
            left.reshape(left.shape[0] * rows, -1), right.reshape(right.shape[0] * rows, -1),
            (((0,), (0,)), ((), ())), preferred_element_type=jnp.float32,
        )
        return product.reshape(count, chunks, ROWS, span).astype(jnp.bfloat16)

    if whole_depth:
        @pl.loop(0, whole_depth)
        def _(at):
            triangle[at] = multiply(wide_left[at], far_right[at])
    if half_depth:
        @pl.loop(0, half_depth)
        def _(at):
            triangle[whole_depth + at] = multiply(half_left[at], half_right[at])

    @pl.loop(0, chunks)
    def _(chunk):
        @pl.loop(1, count)
        def _(step):
            back_copy(chunk, step, me, wrapped(me, step, count)).start()

    def gathered(chunk):
        parts = []
        if whole_depth:
            parts.append(returned[chunk, :, :whole_depth].astype(jnp.float32).reshape(-1, ROWS, span))
        if half_depth:
            near = returned[chunk, :members, whole_depth:].astype(jnp.float32)
            other = returned[chunk, members:, whole_depth:].astype(jnp.float32)
            parts.append((near + other).reshape(-1, ROWS, span))
        return jnp.concatenate(parts, axis=0) if len(parts) > 1 else parts[0]

    @pl.loop(0, chunks)
    def _(chunk):
        @pl.loop(0, depth)
        def _(at):
            returned[chunk, me, at] = triangle[at, me, chunk]

        @pl.loop(1, count)
        def _(step):
            back_copy(chunk, step, wrapped(me, count - step, count), wrapped(me, step, count)).wait()

        standardize(gathered(chunk), plain)

        @pl.loop(0, ROWS)
        def _(row):
            normed = (row_of(plain, row, hidden, span) * wide_gain(1)).astype(jnp.bfloat16)
            inside = inside_of(chunk, row)
            projected = jnp.dot(turned[5], normed, preferred_element_type=jnp.float32)
            gated = inside * gate[chunk * ROWS + row] * projected
            put_row(sided.at[0], row, channels, span, gated)

        pack(sided.at[0], finished.at[chunk], span)

        @pl.loop(1, quads)
        def _(step):
            out_copy(chunk, step, quad, wrapped(quad, step, quads)).start()

        out_keep(chunk).start()

    @pl.loop(0, chunks)
    def _(chunk):
        @pl.loop(1, quads)
        def _(step):
            out_copy(chunk, step, wrapped(quad, quads - step, quads), wrapped(quad, step, quads)).wait()

        out_keep(chunk).wait()


def shards(pair, pair_mask, input_gain, input_weights, out_gate_weight, hidden_gain, out_weight):
    flat = ("gx", "gz")
    quads = lax.axis_size("gz")
    layers = lax.axis_size("gx")
    count = layers * quads
    cores = lax.axis_size("gy")
    local, tall, span = pair.shape
    rows = tall // quads
    chunks = rows // ROWS
    channels = input_gain.shape[0]
    hidden = hidden_gain.shape[0]
    half_depth = 2 * (3 * (hidden // count) // 8) if layers % 2 == 0 else 0
    members = count // 2
    whole_depth = (hidden - half_depth * members) // count
    depth = whole_depth + half_depth
    stay = pl.BlockSpec(memory_space=pltpu.HBM)
    far = pl.BlockSpec(memory_space=pl.ANY)
    copies = pltpu.SemaphoreType.DMA
    tiles = span // LANES
    tallest = max(channels, hidden)
    operands = (
        pair_mask, input_gain[None], input_weights, out_gate_weight, hidden_gain[None], out_weight,
    )
    return pl.pallas_call(
        functools.partial(whole_kernel, flat, count, quads, (whole_depth, half_depth)),
        out_shape=jax.ShapeDtypeStruct(pair.shape, jnp.bfloat16),
        in_specs=[stay] * 7,
        out_specs=far,
        scratch_shapes=[pltpu.VMEM(one.shape, one.dtype) for one in operands] + [
            copies((len(operands),)),
            pltpu.VMEM((6, tallest, tallest), jnp.bfloat16),
            pltpu.VMEM((2, tallest, LANES), jnp.float32),
            pltpu.VMEM((max(whole_depth, 1), count, rows, span * cores), jnp.bfloat16),
            pltpu.VMEM((max(whole_depth, 1), count, rows, span), jnp.bfloat16),
            pltpu.VMEM((max(half_depth, 1), members, rows, span * cores), jnp.bfloat16),
            pltpu.VMEM((max(half_depth, 1), members, rows, span), jnp.bfloat16),
            pltpu.VMEM((rows, channels, span), jnp.float32),
            pltpu.VMEM((depth, count, chunks, ROWS, span), jnp.bfloat16),
            pltpu.VMEM((chunks, channels, ROWS, span), jnp.bfloat16),
            pltpu.VMEM((tiles, tallest * ROWS, LANES), jnp.float32),
            pltpu.VMEM((2, tiles, tallest * ROWS, LANES), jnp.float32),
            pltpu.VMEM((2, chunks, hidden, ROWS, span), jnp.bfloat16),
            pltpu.VMEM((chunks, count, depth, ROWS, span), jnp.bfloat16),
            pltpu.VMEM((chunks, channels, ROWS, span), jnp.bfloat16),
            copies((chunks, quads)),
            copies((chunks, quads)),
            copies((chunks,)),
            copies((2, chunks, count)),
            copies((2, chunks, count)),
            copies((2, chunks, members)),
            copies((2, chunks, members)),
            copies((2, chunks, cores)),
            copies((2, chunks, cores)),
            copies((2, 2, chunks)),
            copies((chunks, count)),
            copies((chunks, count)),
            copies((chunks, quads)),
            copies((chunks, quads)),
            copies((chunks,)),
        ],
        compiler_params=pltpu.CompilerParams(
            collective_id=0, has_side_effects=True, vmem_limit_bytes=40 << 20
        ),
    )(*[pltpu.with_memory_space_constraint(one, pltpu.HBM) for one in (pair, *operands)])


def solution(mesh):
    placed = (P("gz", "gx", "gy"), P("gx", "gy"), P(), P(), P(), P(), P())
    return jax.shard_map(
        shards, mesh=mesh, in_specs=placed, out_specs=P("gz", "gx", "gy"), check_vma=False
    )
```
